128 devices in a mesh: expert: 4 (over y_lo, core), shard: 32 (over z, y_hi, x).
Axes of the slice: x: 4, y: 4 (y_hi: 2, y_lo: 2; y = y_hi * 2 + y_lo), z: 4, core: 2. Of those that a mesh axis runs over, the one named last changes fastest.
Arguments:
- master_gate: float32 [128, 2048, 768], P('expert', 'shard'), may hold values from -0.125 to 0.125
- second_gate: bfloat16 [128, 2048, 768], P('expert', 'shard'), may hold values from -0.0625 to 0.0625
- master_up: float32 [128, 2048, 768], P('expert', 'shard'), may hold values from -0.125 to 0.125
- second_up: bfloat16 [128, 2048, 768], P('expert', 'shard'), may hold values from -0.0625 to 0.0625
- router_weight: float32 [2048, 128], P('shard', 'expert'), may hold values from -0.125 to 0.125
- router_gain: float32 [2048], P('shard'), may hold values from 0.25 to 1.75
Outputs:
- final_gate: bfloat16 [128, 768, 2048], P('expert', 'shard')
- final_up: bfloat16 [128, 768, 2048], P('expert', 'shard')
- serve_router: bfloat16 [2048, 128], replicated
The draws below stay inside these ranges and needn't reach their ends.
All inputs are finite; a program needn't handle non-finite values.
Results may differ from the reference program's by a relative error of at most 0.001.
Values may be sent and summed in bfloat16 or wider, within the bound.
A program may use at most 128 MiB of HBM per device.

```python
import jax
import jax.numpy as jnp

EXPERTS = 128
D_MODEL = 2048
D_EXPERT = 768


def block_levels(own_key, shape, split, low, largest):
    factor_of = 1.0
    for position, parts in split:
        steps = jax.random.uniform(jax.random.fold_in(jax.random.fold_in(own_key, 6), position), (parts,), jnp.float32, low / len(split), largest / len(split))
        factor_of = factor_of * jnp.repeat(jnp.exp(steps), shape[position] // parts).reshape((-1,) + (1,) * (len(shape) - 1 - position))
    return factor_of


def scatter_about(stream_key, dims, width, bound, shards=(), dtype=jnp.bfloat16):
    entries = jax.random.normal(stream_key, dims, jnp.float32) * width
    if len(shards) > 0:
        entries = block_levels(stream_key, dims, shards, -0.22, 0.18) * entries
    return jnp.clip(entries, min=-bound, max=bound).astype(dtype)


def setup_inputs(seed: int = 0) -> dict:
    keys = jax.random.split(jax.random.key(seed), 7)
    master_gate = scatter_about(keys[0], (EXPERTS, D_MODEL, D_EXPERT), D_MODEL ** -0.5, 0.125, ((0, 4), (1, 32)), jnp.float32)
    second_gate = scatter_about(keys[1], (EXPERTS, D_MODEL, D_EXPERT), (D_MODEL * 4) ** -0.5, 0.0625, ((0, 4), (1, 32)))
    master_up = scatter_about(keys[2], (EXPERTS, D_MODEL, D_EXPERT), D_MODEL ** -0.5, 0.125, ((0, 4), (1, 32)), jnp.float32)
    second_up = scatter_about(keys[3], (EXPERTS, D_MODEL, D_EXPERT), (D_MODEL * 4) ** -0.5, 0.0625, ((0, 4), (1, 32)))
    router_weight = scatter_about(keys[4], (D_MODEL, EXPERTS), D_MODEL ** -0.5, 0.125, ((0, 32), (1, 4)), jnp.float32)
    router_gain = jnp.clip(1.0 + 0.15 * jax.random.normal(keys[5], (D_MODEL,), jnp.float32), 0.25, 1.75)
    return {"master_gate": master_gate, "second_gate": second_gate, "master_up": master_up, "second_up": second_up, "router_weight": router_weight, "router_gain": router_gain}


def reference(master_gate, second_gate, master_up, second_up, router_weight, router_gain):
    merged_gate = master_gate + second_gate.astype(jnp.float32)
    merged_up = master_up + second_up.astype(jnp.float32)
    final_gate = merged_gate.astype(jnp.bfloat16)
    final_gate = jnp.transpose(final_gate, (0, 2, 1))
    final_up = merged_up.astype(jnp.bfloat16)
    final_up = jnp.transpose(final_up, (0, 2, 1))
    serve_router = (router_weight * router_gain[:, None]).astype(jnp.bfloat16)
    return final_gate, final_up, serve_router
```

```python
import jax
import jax.numpy as jnp
from jax import lax
from jax.experimental import pallas as pl
from jax.experimental.pallas import tpu as pltpu
from jax.sharding import PartitionSpec as P

MESH = pl.DeviceIdType.MESH
DIM = {"x": 4, "y": 2, "z": 4}
ORDER = (("x", "y", "z"), ("y", "z", "x"), ("z", "x", "y"))
PER = 4
LAG = 2
LANES = 128


def peers_of(dim, pos):
    return [lax.rem(pos[dim] + k, DIM[dim]) for k in range(1, DIM[dim])]


def exchange_kernel(
    chunks, mg, sg, mu, su, rw, rg, gate, up, router,
    s0, s1, s2, a0, a1, a2, b0, b1, b2, c0, c1, c2, mast, sec, rbuf, send, recv, load, rsend, rrecv,
):
    S, R1, R2, R3 = (s0, s1, s2), (a0, a1, a2), (b0, b1, b2), (c0, c1, c2)
    e = lax.axis_index("expert")
    s = lax.axis_index("shard")
    core, y_lo = lax.rem(e, 2), e // 2
    pos = {"x": lax.rem(s, 4), "y": lax.rem(s // 4, 2), "z": s // 8}
    yfull = pos["y"] * 2 + y_lo

    def device(dim, target):
        q = dict(pos)
        q[dim] = target
        return (e, q["z"] * 8 + q["y"] * 4 + q["x"])

    def y_device(target):
        return (lax.rem(target, 2) * 2 + core, pos["z"] * 8 + (target // 2) * 4 + pos["x"])

    partner = (y_lo * 2 + 1 - core, s)

    def loads(ch, slot):
        out = []
        for k, (m, t) in enumerate(((mg, sg), (mu, su))):
            rows = pl.ds(64 * k, 64)
            part = pl.ds(ch * PER, PER)
            out.append(pltpu.make_async_copy(m.at[part], mast.at[slot, :, rows], load.at[slot, 2 * k]))
            out.append(pltpu.make_async_copy(t.at[part], sec.at[slot, :, rows], load.at[slot, 2 * k + 1]))
        return out

    for cp in loads(0, 0):
        cp.start()
    for cp in loads(1, 1):
        cp.start()

    barrier = pltpu.get_barrier_semaphore()
    greet = [device(d, t) for d in "xz" for t in peers_of(d, pos)]
    greet += [y_device(lax.rem(yfull + k, 4)) for k in range(1, 4)]
    greet.append(partner)
    for d in greet:
        pl.semaphore_signal(barrier, inc=1, device_id=d, device_id_type=MESH)

    wide = (rw[...] * rg[...]).T
    tile = jnp.concatenate([wide[16 * g : 16 * g + 16] for g in range(4)], axis=1).astype(jnp.bfloat16)
    rbuf[core, yfull, pos["z"], pos["x"]] = tile

    pl.semaphore_wait(barrier, len(greet))

    def router_copies(phase):
        z, x = pos["z"], pos["x"]
        out = []
        if phase == 0:
            for k, t in enumerate(peers_of("x", pos)):
                ref = rbuf.at[core, yfull, z, x]
                out.append((ref, k, device("x", t)))
        elif phase == 1:
            for k, t in enumerate(peers_of("z", pos)):
                ref = rbuf.at[core, yfull, z]
                out.append((ref, 3 + k, device("z", t)))
        elif phase == 2:
            for k in range(1, 4):
                ref = rbuf.at[core, yfull]
                out.append((ref, 5 + k, y_device(lax.rem(yfull + k, 4))))
        else:
            out.append((rbuf.at[core], 9, partner))
        return [
            pltpu.make_async_remote_copy(r, r, rsend.at[k], rrecv.at[k], device_id=d, device_id_type=MESH)
            for r, k, d in out
        ]

    def router_start(phase):
        for cp in router_copies(phase):
            cp.start()

    def router_wait(phase):
        for cp in router_copies(phase):
            cp.wait()

    router_start(0)

    def copies(p, phase, ch):
        order = ORDER[p]
        dim = order[phase]
        base = sum(DIM[d] - 1 for d in order[:phase])
        out = []
        for k, target in enumerate(peers_of(dim, pos)):
            if phase == 0:
                src, dst = S[p].at[ch, target], R1[p].at[ch, pos[dim]]
            elif phase == 1:
                src, dst = R1[p].at[ch, :, target], R2[p].at[ch, pos[dim]]
            else:
                src, dst = R2[p].at[ch, :, :, target], R3[p].at[ch, pos[dim]]
            out.append(
                pltpu.make_async_remote_copy(
                    src, dst, send.at[p, ch, base + k], recv.at[p, ch, base + k],
                    device_id=device(dim, target), device_id_type=MESH,
                )
            )
        return out

    def merge(ch):
        slot = lax.rem(ch, 2)
        for cp in loads(ch, slot):
            cp.wait()

        def pair(j, _):
            for b in range(6):
                lanes = slice(LANES * b, LANES * (b + 1))
                turned = [
                    (mast[slot, 2 * j + i, :, lanes] + sec[slot, 2 * j + i, :, lanes].astype(jnp.float32)).T
                    for i in range(2)
                ]
                for g in range(16):
                    group = 16 * b + g
                    to, p = group // 3, group % 3
                    at = {"x": to % 4, "y": (to // 4) % 2, "z": to // 8}
                    block = jnp.concatenate([t[8 * g : 8 * g + 8] for t in turned], axis=0).astype(jnp.bfloat16)
                    d0, d1, d2 = (at[d] for d in ORDER[p])
                    S[p][ch, d0, d1, d2, pl.ds(pl.multiple_of(16 * j, 16), 16), :] = block
            return 0

        lax.fori_loop(0, PER // 2, pair, 0)

        @pl.when(ch + 2 < chunks)
        def _():
            for cp in loads(ch + 2, slot):
                cp.start()

    def begin(phase, ch):
        for p in range(3):
            for cp in copies(p, phase, ch):
                cp.start()
        for p in range(3):
            own = pos[ORDER[p][phase]]
            if phase == 0:
                R1[p][ch, own] = S[p][ch, own]
            elif phase == 1:
                R2[p][ch, own] = R1[p][ch, :, own]
            else:
                R3[p][ch, own] = R2[p][ch, :, :, own]

    def arrive(phase, ch):
        for p in range(3):
            for cp in copies(p, phase, ch):
                cp.wait_recv()

    def assemble(ch):
        def pair(j, _):
            rows = pl.ds(pl.multiple_of(16 * j, 16), 16)
            for p in range(3):
                for q in range(16):
                    halves = []
                    for src in (2 * q, 2 * q + 1):
                        at = {"x": src % 4, "y": (src // 4) % 2, "z": src // 8}
                        d0, d1, d2 = (at[d] for d in ORDER[p])
                        halves.append(R3[p][ch, d2, d1, d0, rows, :])
                    for out, cut in ((gate, slice(0, 64)), (up, slice(64, 128))):
                        whole = jnp.concatenate([h[:, cut] for h in halves], axis=1)
                        for i in range(2):
                            out[ch * PER + 2 * j + i, 8 * p : 8 * p + 8, LANES * q : LANES * (q + 1)] = whole[
                                8 * i : 8 * i + 8
                            ]
            return 0

        lax.fori_loop(0, PER // 2, pair, 0)

    def step(t, _):
        @pl.when(t < chunks)
        def _():
            merge(t)
            begin(0, t)

        for ph in range(1, 4):
            @pl.when(t == ph)
            def _():
                router_wait(ph - 1)
                router_start(ph)

        @pl.when((t >= LAG) & (t < chunks + LAG))
        def _():
            arrive(0, t - LAG)
            begin(1, t - LAG)

        @pl.when((t >= 2 * LAG) & (t < chunks + 2 * LAG))
        def _():
            arrive(1, t - 2 * LAG)
            begin(2, t - 2 * LAG)

        @pl.when(t >= 3 * LAG)
        def _():
            arrive(2, t - 3 * LAG)
            assemble(t - 3 * LAG)

        @pl.when(t == 6)
        def _():
            router_wait(3)

            def rows(i, _):
                z, y, x = i // 8, lax.rem(i // 4, 2), lax.rem(i, 4)
                tiles = [rbuf[k % 2, 2 * y + k // 2, z, x] for k in range(4)]
                for g in range(4):
                    block = jnp.concatenate([w[:, 32 * g : 32 * g + 32] for w in tiles], axis=1)
                    router[pl.ds(pl.multiple_of(64 * i + 16 * g, 16), 16), :] = block
                return 0

            lax.fori_loop(0, 32, rows, 0)

        return 0

    lax.fori_loop(0, chunks + 3 * LAG, step, 0)

    def drain(ch, _):
        for phase in range(3):
            for p in range(3):
                for cp in copies(p, phase, ch):
                    cp.wait_send()
        return 0

    lax.fori_loop(0, chunks, drain, 0)


def per_device(master_gate, second_gate, master_up, second_up, router_weight, router_gain):
    experts, rows, width = master_gate.shape
    chunks = experts // PER
    block = (PER * 8, LANES)

    def held(dims):
        return pltpu.VMEM((chunks,) + tuple(DIM[d] for d in dims) + block, jnp.bfloat16)

    any_ = pl.BlockSpec(memory_space=pl.ANY)
    vmem = pl.BlockSpec(memory_space=pltpu.VMEM)
    out = (experts, width // 32, rows * 32)
    return pl.pallas_call(
        lambda *refs: exchange_kernel(chunks, *refs),
        name="merge_exchange",
        out_shape=(
            pltpu.VMEM(out, jnp.bfloat16),
            pltpu.VMEM(out, jnp.bfloat16),
            pltpu.VMEM((rows * 32, 128), jnp.bfloat16),
        ),
        in_specs=[any_] * 4 + [vmem] * 2,
        out_specs=(vmem, vmem, vmem),
        scratch_shapes=[held(o) for o in ORDER]
        + [held(o) for o in ORDER]
        + [held((o[1], o[0], o[2])) for o in ORDER]
        + [held((o[2], o[1], o[0])) for o in ORDER]
        + [
            pltpu.VMEM((2, PER, 2 * rows, width), jnp.float32),
            pltpu.VMEM((2, PER, 2 * rows, width), jnp.bfloat16),
            pltpu.VMEM((2, 4, 4, 4, 16, LANES), jnp.bfloat16),
            pltpu.SemaphoreType.DMA((3, chunks, 7)),
            pltpu.SemaphoreType.DMA((3, chunks, 7)),
            pltpu.SemaphoreType.DMA((2, 4)),
            pltpu.SemaphoreType.DMA((10,)),
            pltpu.SemaphoreType.DMA((10,)),
        ],
        compiler_params=pltpu.CompilerParams(
            collective_id=0, has_side_effects=True, vmem_limit_bytes=56 * 1024 * 1024
        ),
    )(master_gate, second_gate, master_up, second_up, router_weight.T, router_gain[None, :])


def solution(mesh):
    placed = (
        P("expert", "shard", None),
        P("expert", "shard", None),
        P("expert", "shard", None),
        P("expert", "shard", None),
        P("shard", "expert"),
        P("shard"),
    )
    return jax.shard_map(
        per_device,
        mesh=mesh,
        in_specs=placed,
        out_specs=(P("expert", "shard", None), P("expert", "shard", None), P()),
        check_vma=False,
    )
```

```python
import jax
import jax.numpy as jnp
from jax import lax
from jax.experimental import pallas as pl
from jax.experimental.pallas import tpu as pltpu
from jax.sharding import PartitionSpec as P

MESH = pl.DeviceIdType.MESH
DIM = {"x": 4, "y": 2, "z": 4}
ORDER = (("x", "y", "z"), ("y", "z", "x"), ("z", "x", "y"))
UNIT = 2
CHUNKS = (2, 4, 4, 4, 2)
LAG = 1
ROUTER_STEPS = (1, 2, 4, 5)
LANES = 128


def peers_of(dim, pos):
    return [lax.rem(pos[dim] + k, DIM[dim]) for k in range(1, DIM[dim])]


def exchange_kernel(
    chunks, mg, sg, mu, su, rw, rg, gate, up, router,
    s0, s1, s2, a0, a1, a2, b0, b1, b2, c0, c1, c2, mast, sec, rbuf, send, recv, load, rsend, rrecv,
):
    count = len(chunks)
    starts = [sum(chunks[:c]) for c in range(count)]
    S, R1, R2, R3 = (s0, s1, s2), (a0, a1, a2), (b0, b1, b2), (c0, c1, c2)
    e = lax.axis_index("expert")
    s = lax.axis_index("shard")
    core, y_lo = lax.rem(e, 2), e // 2
    pos = {"x": lax.rem(s, 4), "y": lax.rem(s // 4, 2), "z": s // 8}
    yfull = pos["y"] * 2 + y_lo

    def device(dim, target):
        q = dict(pos)
        q[dim] = target
        return (e, q["z"] * 8 + q["y"] * 4 + q["x"])

    def y_device(target):
        return (lax.rem(target, 2) * 2 + core, pos["z"] * 8 + (target // 2) * 4 + pos["x"])

    partner = (y_lo * 2 + 1 - core, s)

    def loads(ch):
        out = []
        part = pl.ds(starts[ch] * UNIT, chunks[ch] * UNIT)
        for k, (m, t) in enumerate(((mg, sg), (mu, su))):
            rows = pl.ds(64 * k, 64)
            out.append(pltpu.make_async_copy(m.at[part], mast.at[part, rows], load.at[ch, 2 * k]))
            out.append(pltpu.make_async_copy(t.at[part], sec.at[part, rows], load.at[ch, 2 * k + 1]))
        return out

    for ch in range(2):
        for cp in loads(ch):
            cp.start()

    barrier = pltpu.get_barrier_semaphore()
    greet = [device(d, t) for d in "xz" for t in peers_of(d, pos)]
    greet += [y_device(lax.rem(yfull + k, 4)) for k in range(1, 4)]
    greet.append(partner)
    for d in greet:
        pl.semaphore_signal(barrier, inc=1, device_id=d, device_id_type=MESH)

    wide = (rw[...] * rg[...]).T
    tile = jnp.concatenate([wide[16 * g : 16 * g + 16] for g in range(4)], axis=1).astype(jnp.bfloat16)
    rbuf[core, yfull, pos["z"], pos["x"]] = tile

    pl.semaphore_wait(barrier, len(greet))

    def router_copies(phase, first):
        z, x = pos["z"], pos["x"]
        out = []
        if phase == 0:
            for k, t in enumerate(peers_of("x", pos)):
                out.append((rbuf.at[core, yfull, z, x], k, device("x", t)))
        elif phase == 3:
            out.append((rbuf.at[core], 9, partner))
        elif (phase == 1) == (first == "z"):
            ref = rbuf.at[core, yfull, z] if first == "z" else rbuf.at[core, :, z]
            for k, t in enumerate(peers_of("z", pos)):
                out.append((ref, 3 + k, device("z", t)))
        else:
            ref = rbuf.at[core, yfull, z] if first == "y" else rbuf.at[core, yfull]
            for k in range(1, 4):
                out.append((ref, 5 + k, y_device(lax.rem(yfull + k, 4))))
        return [
            pltpu.make_async_remote_copy(r, r, rsend.at[k], rrecv.at[k], device_id=d, device_id_type=MESH)
            for r, k, d in out
        ]

    def router_step(done, start):
        for index, first in enumerate(("z", "y")):

            @pl.when(core == index)
            def _():
                if done is not None:
                    for cp in router_copies(done, first):
                        cp.wait()
                if start is not None:
                    for cp in router_copies(start, first):
                        cp.start()

    router_step(None, 0)

    def copies(p, phase, ch):
        order = ORDER[p]
        dim = order[phase]
        base = sum(DIM[d] - 1 for d in order[:phase])
        part = pl.ds(starts[ch], chunks[ch])
        out = []
        for k, target in enumerate(peers_of(dim, pos)):
            if phase == 0:
                src, dst = S[p].at[part, target], R1[p].at[part, pos[dim]]
            elif phase == 1:
                src, dst = R1[p].at[part, :, target], R2[p].at[part, pos[dim]]
            else:
                src, dst = R2[p].at[part, :, :, target], R3[p].at[part, pos[dim]]
            out.append(
                pltpu.make_async_remote_copy(
                    src, dst, send.at[p, ch, base + k], recv.at[p, ch, base + k],
                    device_id=device(dim, target), device_id_type=MESH,
                )
            )
        return out

    def merge(ch):
        for cp in loads(ch):
            cp.wait()
        if ch + 2 < count:
            for cp in loads(ch + 2):
                cp.start()

        def unit(j, _):
            for b in range(6):
                lanes = slice(LANES * b, LANES * (b + 1))
                turned = [
                    (mast[UNIT * j + i, :, lanes] + sec[UNIT * j + i, :, lanes].astype(jnp.float32)).T
                    for i in range(UNIT)
                ]
                for g in range(16):
                    group = 16 * b + g
                    to, p = group // 3, group % 3
                    at = {"x": to % 4, "y": (to // 4) % 2, "z": to // 8}
                    block = jnp.concatenate([t[8 * g : 8 * g + 8] for t in turned], axis=0).astype(jnp.bfloat16)
                    d0, d1, d2 = (at[d] for d in ORDER[p])
                    S[p][j, d0, d1, d2] = block
            return 0

        lax.fori_loop(starts[ch], starts[ch] + chunks[ch], unit, 0)

    def begin(phase, ch):
        for p in range(3):
            for cp in copies(p, phase, ch):
                cp.start()

        def unit(j, _):
            for p in range(3):
                own = pos[ORDER[p][phase]]
                if phase == 0:
                    R1[p][j, own] = S[p][j, own]
                elif phase == 1:
                    R2[p][j, own] = R1[p][j, :, own]
                else:
                    R3[p][j, own] = R2[p][j, :, :, own]
            return 0

        lax.fori_loop(starts[ch], starts[ch] + chunks[ch], unit, 0)

    def arrive(phase, ch):
        for p in range(3):
            for cp in copies(p, phase, ch):
                cp.wait_recv()

    def assemble(ch):
        def unit(j, _):
            for p in range(3):
                for q in range(16):
                    halves = []
                    for src in (2 * q, 2 * q + 1):
                        at = {"x": src % 4, "y": (src // 4) % 2, "z": src // 8}
                        d0, d1, d2 = (at[d] for d in ORDER[p])
                        halves.append(R3[p][j, d2, d1, d0])
                    for out, cut in ((gate, slice(0, 64)), (up, slice(64, 128))):
                        whole = jnp.concatenate([h[:, cut] for h in halves], axis=1)
                        for i in range(UNIT):
                            out[UNIT * j + i, 8 * p : 8 * p + 8, LANES * q : LANES * (q + 1)] = whole[
                                8 * i : 8 * i + 8
                            ]
            return 0

        lax.fori_loop(starts[ch], starts[ch] + chunks[ch], unit, 0)

    def finish_router():
        def rows(i, _):
            z, y, x = i // 8, lax.rem(i // 4, 2), lax.rem(i, 4)
            tiles = [rbuf[k % 2, 2 * y + k // 2, z, x] for k in range(4)]
            for g in range(4):
                block = jnp.concatenate([w[:, 32 * g : 32 * g + 32] for w in tiles], axis=1)
                router[pl.ds(pl.multiple_of(64 * i + 16 * g, 16), 16), :] = block
            return 0

        lax.fori_loop(0, 32, rows, 0)

    for t in range(count + 3 * LAG):
        if t < count:
            merge(t)
            begin(0, t)
        if 0 <= t - LAG < count:
            arrive(0, t - LAG)
            begin(1, t - LAG)
        if 0 <= t - 2 * LAG < count:
            arrive(1, t - 2 * LAG)
            begin(2, t - 2 * LAG)
        if 0 <= t - 3 * LAG < count:
            arrive(2, t - 3 * LAG)
            assemble(t - 3 * LAG)
        if t in ROUTER_STEPS:
            phase = ROUTER_STEPS.index(t)
            router_step(phase, phase + 1 if phase < 3 else None)
            if phase == 3:
                finish_router()

    for ch in range(count):
        for phase in range(3):
            for p in range(3):
                for cp in copies(p, phase, ch):
                    cp.wait_send()


def store_kernel(gate, up, router, gate_out, up_out, router_out, sem):
    copies = [
        pltpu.make_async_copy(gate, gate_out, sem.at[0]),
        pltpu.make_async_copy(up, up_out, sem.at[1]),
        pltpu.make_async_copy(router, router_out, sem.at[2]),
    ]
    for cp in copies:
        cp.start()
    for cp in copies:
        cp.wait()


def per_device(master_gate, second_gate, master_up, second_up, router_weight, router_gain):
    experts, rows, width = master_gate.shape
    units = experts // UNIT
    chunks = CHUNKS

    def held(dims):
        return pltpu.VMEM((units,) + tuple(DIM[d] for d in dims) + (8 * UNIT, LANES), jnp.bfloat16)

    any_ = pl.BlockSpec(memory_space=pl.ANY)
    vmem = pl.BlockSpec(memory_space=pltpu.VMEM)
    shapes = [(experts, width // 32, rows * 32)] * 2 + [(rows * 32, 128)]
    outs = pl.pallas_call(
        lambda *refs: exchange_kernel(chunks, *refs),
        name="merge_exchange",
        out_shape=tuple(pltpu.VMEM(shape, jnp.bfloat16) for shape in shapes),
        in_specs=[any_] * 4 + [vmem] * 2,
        out_specs=(vmem, vmem, vmem),
        scratch_shapes=[held(o) for o in ORDER]
        + [held(o) for o in ORDER]
        + [held((o[1], o[0], o[2])) for o in ORDER]
        + [held((o[2], o[1], o[0])) for o in ORDER]
        + [
            pltpu.VMEM((experts, 2 * rows, width), jnp.float32),
            pltpu.VMEM((experts, 2 * rows, width), jnp.bfloat16),
            pltpu.VMEM((2, 4, 4, 4, 16, LANES), jnp.bfloat16),
            pltpu.SemaphoreType.DMA((3, len(chunks), 7)),
            pltpu.SemaphoreType.DMA((3, len(chunks), 7)),
            pltpu.SemaphoreType.DMA((len(chunks), 4)),
            pltpu.SemaphoreType.DMA((10,)),
            pltpu.SemaphoreType.DMA((10,)),
        ],
        compiler_params=pltpu.CompilerParams(
            collective_id=0, has_side_effects=True, vmem_limit_bytes=48 * 1024 * 1024
        ),
    )(master_gate, second_gate, master_up, second_up, router_weight.T, router_gain[None, :])
    return pl.pallas_call(
        store_kernel,
        name="store",
        out_shape=tuple(jax.ShapeDtypeStruct(shape, jnp.bfloat16) for shape in shapes),
        in_specs=[vmem] * 3,
        out_specs=(any_,) * 3,
        scratch_shapes=[pltpu.SemaphoreType.DMA((3,))],
        compiler_params=pltpu.CompilerParams(vmem_limit_bytes=16 * 1024 * 1024),
    )(*(pltpu.with_memory_space_constraint(out, pltpu.VMEM) for out in outs))


def solution(mesh):
    placed = (
        P("expert", "shard", None),
        P("expert", "shard", None),
        P("expert", "shard", None),
        P("expert", "shard", None),
        P("shard", "expert"),
        P("shard"),
    )
    return jax.shard_map(
        per_device,
        mesh=mesh,
        in_specs=placed,
        out_specs=(P("expert", "shard", None), P("expert", "shard", None), P()),
        check_vma=False,
    )
```

```python
import jax
import jax.numpy as jnp
from jax import lax
from jax.experimental import pallas as pl
from jax.experimental.pallas import tpu as pltpu
from jax.sharding import PartitionSpec as P

MESH = pl.DeviceIdType.MESH
DIM = {"x": 4, "y": 2, "z": 4}
ORDER = (("x", "y", "z"), ("y", "z", "x"), ("z", "x", "y"))
UNIT = 2
CHUNKS = (2, 4, 4, 4, 2)
ROUTER_STEPS = (1, 2, 4, 5)
ROUTER_ORDER = (("x", "y", "z"), ("z", "y", "x"))
LANES = 128


def peers_of(dim, pos):
    return [lax.rem(pos[dim] + k, DIM[dim]) for k in range(1, DIM[dim])]


def assemble(first, units, pieces, gate, up):
    def unit(j, _):
        for p in range(3):
            for q in range(16):
                halves = []
                for src in (2 * q, 2 * q + 1):
                    at = {"x": src % 4, "y": (src // 4) % 2, "z": src // 8}
                    d0, d1, d2 = (at[d] for d in ORDER[p])
                    halves.append(pieces[p][j, d2, d1, d0])
                for out, cut in ((gate, slice(0, 64)), (up, slice(64, 128))):
                    whole = jnp.concatenate([h[:, cut] for h in halves], axis=1)
                    for i in range(UNIT):
                        out[UNIT * j + i, 8 * p : 8 * p + 8, LANES * q : LANES * (q + 1)] = whole[8 * i : 8 * i + 8]
        return 0

    lax.fori_loop(first, first + units, unit, 0)


def exchange_kernel(
    chunks, mg, sg, mu, su, rw, rg, gate, up, router, e0, e1, e2,
    s0, s1, s2, a0, a1, a2, b0, b1, b2, c0, c1, c2, mast, sec, rbuf, weight, gain, send, recv, load, rload, rsend, rrecv,
):
    count = len(chunks)
    starts = [sum(chunks[:c]) for c in range(count)]
    S, R1, R2, R3, LAST = (s0, s1, s2), (a0, a1, a2), (b0, b1, b2), (c0, c1, c2), (e0, e1, e2)
    e = lax.axis_index("expert")
    s = lax.axis_index("shard")
    core, y_lo = lax.rem(e, 2), e // 2
    pos = {"x": lax.rem(s, 4), "y": lax.rem(s // 4, 2), "z": s // 8}
    yfull = pos["y"] * 2 + y_lo

    def device(dim, target):
        q = dict(pos)
        q[dim] = target
        return (e, q["z"] * 8 + q["y"] * 4 + q["x"])

    def y_device(target):
        return (lax.rem(target, 2) * 2 + core, pos["z"] * 8 + (target // 2) * 4 + pos["x"])

    partner = (y_lo * 2 + 1 - core, s)

    def loads(ch):
        part = pl.ds(starts[ch] * UNIT, chunks[ch] * UNIT)
        for k, (m, t) in enumerate(((mg, sg), (mu, su))):
            rows = pl.ds(64 * k, 64)
            pltpu.make_async_copy(m.at[part], mast.at[part, rows], load.at[ch, 0]).start()
            pltpu.make_async_copy(t.at[part], sec.at[part, rows], load.at[ch, 1]).start()

    def loaded(ch):
        part = pl.ds(starts[ch] * UNIT, chunks[ch] * UNIT)
        pltpu.make_async_copy(mast.at[part], mast.at[part], load.at[ch, 0]).wait()
        pltpu.make_async_copy(sec.at[part], sec.at[part], load.at[ch, 1]).wait()

    small = [pltpu.make_async_copy(rw, weight, rload.at[0]), pltpu.make_async_copy(rg, gain, rload.at[1])]
    for cp in small:
        cp.start()
    loads(0)
    loads(1)

    barrier = pltpu.get_barrier_semaphore()
    greet = [device(d, t) for d in "xz" for t in peers_of(d, pos)]
    greet += [y_device(lax.rem(yfull + k, 4)) for k in range(1, 4)]
    greet.append(partner)
    for d in greet:
        pl.semaphore_signal(barrier, inc=1, device_id=d, device_id_type=MESH)

    def router_tile():
        for cp in small:
            cp.wait()
        wide = (weight[...] * gain[...]).T
        tile = jnp.concatenate([wide[16 * g : 16 * g + 16] for g in range(4)], axis=1).astype(jnp.bfloat16)
        rbuf[core, yfull, pos["z"], pos["x"]] = tile

    def router_phase(phase, dims):
        at = {"x": pos["x"], "y": yfull, "z": pos["z"]}
        if phase == 3:
            return [(rbuf.at[core], partner)], rbuf.at[1 - core]
        known = dims[:phase]
        index = tuple(slice(None) if d in known else at[d] for d in "yzx")
        ref = rbuf.at[(core,) + index]
        dim = dims[phase]
        to = [y_device(lax.rem(yfull + k, 4)) for k in range(1, 4)] if dim == "y" else [
            device(dim, t) for t in peers_of(dim, pos)
        ]
        wide = tuple(pl.ds(0, 3) if d == dim else (slice(None) if d in known else 0) for d in "yzx")
        return [(ref, d) for d in to], rbuf.at[(core,) + wide]

    def router_step(done, start):
        for index, dims in enumerate(ROUTER_ORDER):

            @pl.when(core == index)
            def _():
                if done is not None:
                    _, view = router_phase(done, dims)
                    whole = pltpu.make_async_remote_copy(
                        view, view, rsend.at[done], rrecv.at[done], device_id=partner, device_id_type=MESH
                    )
                    whole.wait()
                if start is not None:
                    for ref, d in router_phase(start, dims)[0]:
                        pltpu.make_async_remote_copy(
                            ref, ref, rsend.at[start], rrecv.at[start], device_id=d, device_id_type=MESH
                        ).start()

    def copies(p, phase, ch):
        order = ORDER[p]
        dim = order[phase]
        part = pl.ds(starts[ch], chunks[ch])
        out = []
        for target in peers_of(dim, pos):
            if phase == 0:
                src, dst = S[p].at[part, target], R1[p].at[part, pos[dim]]
            elif phase == 1:
                src, dst = R1[p].at[part, :, target], R2[p].at[part, pos[dim]]
            else:
                src = R2[p].at[part, :, :, target]
                dst = R3[p].at[part, pos[dim]] if ch + 1 < count else LAST[p].at[:, pos[dim]]
            out.append(
                pltpu.make_async_remote_copy(
                    src, dst, send.at[0], recv.at[phase, ch], device_id=device(dim, target), device_id_type=MESH
                )
            )
        return out

    def merge(ch):
        loaded(ch)
        if ch + 2 < count:
            loads(ch + 2)

        def unit(j, _):
            for b in range(6):
                lanes = slice(LANES * b, LANES * (b + 1))
                turned = [
                    (mast[UNIT * j + i, :, lanes] + sec[UNIT * j + i, :, lanes].astype(jnp.float32)).T
                    for i in range(UNIT)
                ]
                for g in range(16):
                    group = 16 * b + g
                    to, p = group // 3, group % 3
                    at = {"x": to % 4, "y": (to // 4) % 2, "z": to // 8}
                    block = jnp.concatenate([t[8 * g : 8 * g + 8] for t in turned], axis=0).astype(jnp.bfloat16)
                    d0, d1, d2 = (at[d] for d in ORDER[p])
                    S[p][j, d0, d1, d2] = block
            return 0

        lax.fori_loop(starts[ch], starts[ch] + chunks[ch], unit, 0)

    def begin(phase, ch):
        for p in range(3):
            for cp in copies(p, phase, ch):
                cp.start()

        def unit(j, _):
            for p in range(3):
                own = pos[ORDER[p][phase]]
                if phase == 0:
                    R1[p][j, own] = S[p][j, own]
                elif phase == 1:
                    R2[p][j, own] = R1[p][j, :, own]
                elif ch + 1 < count:
                    R3[p][j, own] = R2[p][j, :, :, own]
                else:
                    LAST[p][j - starts[ch], own] = R2[p][j, :, :, own]
            return 0

        lax.fori_loop(starts[ch], starts[ch] + chunks[ch], unit, 0)

    def arrive(phase, ch):
        view = sec.at[pl.ds(starts[ch] * UNIT, chunks[ch] * UNIT), :, pl.ds(0, 512)]
        pltpu.make_async_copy(view, view, recv.at[phase, ch]).wait()

    def finish_router():
        def rows(i, _):
            z, y, x = i // 8, lax.rem(i // 4, 2), lax.rem(i, 4)
            tiles = [rbuf[k % 2, 2 * y + k // 2, z, x] for k in range(4)]
            for g in range(4):
                block = jnp.concatenate([w[:, 32 * g : 32 * g + 32] for w in tiles], axis=1)
                router[pl.ds(pl.multiple_of(64 * i + 16 * g, 16), 16), :] = block
            return 0

        lax.fori_loop(0, 32, rows, 0)

    router_tile()
    merge(0)
    pl.semaphore_wait(barrier, len(greet))
    begin(0, 0)
    router_step(None, 0)

    for t in range(1, count + 3):
        if t < count:
            merge(t)
            begin(0, t)
        if t <= count:
            arrive(0, t - 1)
            begin(1, t - 1)
        if 0 <= t - 2 < count:
            arrive(1, t - 2)
            begin(2, t - 2)
        if t in ROUTER_STEPS:
            phase = ROUTER_STEPS.index(t)
            router_step(phase, phase + 1 if phase < 3 else None)
            if phase == 3:
                finish_router()
        if t >= 3:
            arrive(2, t - 3)
            if t - 2 < count:
                assemble(starts[t - 3], chunks[t - 3], R3, gate, up)

    pltpu.make_async_copy(mast, mast, send.at[0]).wait()


def store_kernel(gate, up, router, e0, e1, e2, gate_out, up_out, router_out, gate_last, up_last, sem):
    done, last = gate.shape[0], gate_last.shape[0]
    copies = [
        pltpu.make_async_copy(gate, gate_out.at[pl.ds(0, done)], sem.at[0]),
        pltpu.make_async_copy(up, up_out.at[pl.ds(0, done)], sem.at[1]),
        pltpu.make_async_copy(router, router_out, sem.at[2]),
        pltpu.make_async_copy(gate_last, gate_out.at[pl.ds(done, last)], sem.at[3]),
        pltpu.make_async_copy(up_last, up_out.at[pl.ds(done, last)], sem.at[4]),
    ]
    for cp in copies[:3]:
        cp.start()
    assemble(0, last // UNIT, (e0, e1, e2), gate_last, up_last)
    for cp in copies[3:]:
        cp.start()
    for cp in copies:
        cp.wait()


def per_device(master_gate, second_gate, master_up, second_up, router_weight, router_gain):
    experts, rows, width = master_gate.shape
    units = experts // UNIT
    chunks = CHUNKS

    last = chunks[-1]

    def held(dims, count=units):
        return pltpu.VMEM((count,) + tuple(DIM[d] for d in dims) + (8 * UNIT, LANES), jnp.bfloat16)

    any_ = pl.BlockSpec(memory_space=pl.ANY)
    vmem = pl.BlockSpec(memory_space=pltpu.VMEM)
    shapes = [(experts, width // 32, rows * 32)] * 2 + [(rows * 32, 128)]
    outs = pl.pallas_call(
        lambda *refs: exchange_kernel(chunks, *refs),
        name="merge_exchange",
        out_shape=tuple(pltpu.VMEM((experts - UNIT * last,) + shape[1:], jnp.bfloat16) for shape in shapes[:2])
        + (pltpu.VMEM(shapes[2], jnp.bfloat16),)
        + tuple(held((o[2], o[1], o[0]), last) for o in ORDER),
        in_specs=[any_] * 6,
        out_specs=(vmem,) * 6,
        scratch_shapes=[held(o) for o in ORDER]
        + [held(o) for o in ORDER]
        + [held((o[1], o[0], o[2])) for o in ORDER]
        + [held((o[2], o[1], o[0]), units - last) for o in ORDER]
        + [
            pltpu.VMEM((experts, 2 * rows, width), jnp.float32),
            pltpu.VMEM((experts, 2 * rows, width), jnp.bfloat16),
            pltpu.VMEM((2, 4, 4, 4, 16, LANES), jnp.bfloat16),
            pltpu.VMEM((rows // 2, rows), jnp.float32),
            pltpu.VMEM((1, rows), jnp.float32),
            pltpu.SemaphoreType.DMA((1,)),
            pltpu.SemaphoreType.DMA((3, len(chunks))),
            pltpu.SemaphoreType.DMA((len(chunks), 2)),
            pltpu.SemaphoreType.DMA((2,)),
            pltpu.SemaphoreType.DMA((4,)),
            pltpu.SemaphoreType.DMA((4,)),
        ],
        compiler_params=pltpu.CompilerParams(
            collective_id=0, has_side_effects=True, vmem_limit_bytes=48 * 1024 * 1024
        ),
    )(master_gate, second_gate, master_up, second_up, router_weight.T, router_gain[None, :])
    return pl.pallas_call(
        store_kernel,
        name="store",
        out_shape=tuple(jax.ShapeDtypeStruct(shape, jnp.bfloat16) for shape in shapes),
        in_specs=[vmem] * 6,
        out_specs=(any_,) * 3,
        scratch_shapes=[pltpu.VMEM((UNIT * last,) + shape[1:], jnp.bfloat16) for shape in shapes[:2]]
        + [pltpu.SemaphoreType.DMA((5,))],
        compiler_params=pltpu.CompilerParams(vmem_limit_bytes=16 * 1024 * 1024),
    )(*(pltpu.with_memory_space_constraint(out, pltpu.VMEM) for out in outs))


def solution(mesh):
    placed = (
        P("expert", "shard", None),
        P("expert", "shard", None),
        P("expert", "shard", None),
        P("expert", "shard", None),
        P("shard", "expert"),
        P("shard"),
    )
    return jax.shard_map(
        per_device,
        mesh=mesh,
        in_specs=placed,
        out_specs=(P("expert", "shard", None), P("expert", "shard", None), P()),
        check_vma=False,
    )
```

```python
import jax
import jax.numpy as jnp
from jax import lax
from jax.experimental import pallas as pl
from jax.experimental.pallas import tpu as pltpu
from jax.sharding import PartitionSpec as P

MESH = pl.DeviceIdType.MESH
DIM = {"x": 4, "y": 2, "z": 4}
ORDER = (("x", "y", "z"), ("y", "z", "x"), ("z", "x", "y"))
UNIT = 2
CHUNKS = (2, 4, 4, 4, 2)
ROUTER_STEPS = (1, 2, 4, 5)
ROUTER_ORDER = (("x", "y", "z"), ("z", "y", "x"))
LANES = 128


def peers_of(dim, pos):
    return [lax.rem(pos[dim] + k, DIM[dim]) for k in ((2, 1, 3) if DIM[dim] == 4 else (1,))]


def assemble(first, units, pieces, gate, up):
    def unit(j, _):
        for p in range(3):
            for q in range(16):
                halves = []
                for src in (2 * q, 2 * q + 1):
                    at = {"x": src % 4, "y": (src // 4) % 2, "z": src // 8}
                    d0, d1, d2 = (at[d] for d in ORDER[p])
                    halves.append(pieces[p][j, d2, d1, d0])
                for out, cut in ((gate, slice(0, 64)), (up, slice(64, 128))):
                    whole = jnp.concatenate([h[:, cut] for h in halves], axis=1)
                    for i in range(UNIT):
                        out[UNIT * j + i, 8 * p : 8 * p + 8, LANES * q : LANES * (q + 1)] = whole[8 * i : 8 * i + 8]
        return 0

    lax.fori_loop(first, first + units, unit, 0)


def exchange_kernel(
    chunks, mg, sg, mu, su, rw, rg, gate, up, router, e0, e1, e2,
    s0, s1, s2, a0, a1, a2, b0, b1, b2, c0, c1, c2, mast, sec, rbuf, weight, gain, send, recv, load, rload, rsend, rrecv,
):
    count = len(chunks)
    starts = [sum(chunks[:c]) for c in range(count)]
    S, R1, R2, R3, LAST = (s0, s1, s2), (a0, a1, a2), (b0, b1, b2), (c0, c1, c2), (e0, e1, e2)
    e = lax.axis_index("expert")
    s = lax.axis_index("shard")
    core, y_lo = lax.rem(e, 2), e // 2
    pos = {"x": lax.rem(s, 4), "y": lax.rem(s // 4, 2), "z": s // 8}
    yfull = pos["y"] * 2 + y_lo

    def device(dim, target):
        q = dict(pos)
        q[dim] = target
        return (e, q["z"] * 8 + q["y"] * 4 + q["x"])

    def y_device(target):
        return (lax.rem(target, 2) * 2 + core, pos["z"] * 8 + (target // 2) * 4 + pos["x"])

    partner = (y_lo * 2 + 1 - core, s)

    def loads(ch):
        part = pl.ds(starts[ch] * UNIT, chunks[ch] * UNIT)
        for k, (m, t) in enumerate(((mg, sg), (mu, su))):
            rows = pl.ds(64 * k, 64)
            pltpu.make_async_copy(m.at[part], mast.at[part, rows], load.at[ch, 0]).start()
            pltpu.make_async_copy(t.at[part], sec.at[part, rows], load.at[ch, 1]).start()

    def loaded(ch):
        part = pl.ds(starts[ch] * UNIT, chunks[ch] * UNIT)
        pltpu.make_async_copy(mast.at[part], mast.at[part], load.at[ch, 0]).wait()
        pltpu.make_async_copy(sec.at[part], sec.at[part], load.at[ch, 1]).wait()

    small = [pltpu.make_async_copy(rw, weight, rload.at[0]), pltpu.make_async_copy(rg, gain, rload.at[1])]
    for cp in small:
        cp.start()
    loads(0)
    loads(1)

    barrier = pltpu.get_barrier_semaphore()
    greet = [device(d, t) for d in "xz" for t in peers_of(d, pos)]
    greet += [y_device(lax.rem(yfull + k, 4)) for k in range(1, 4)]
    greet.append(partner)
    for d in greet:
        pl.semaphore_signal(barrier, inc=1, device_id=d, device_id_type=MESH)

    def router_tile():
        for cp in small:
            cp.wait()
        wide = (weight[...] * gain[...]).T
        tile = jnp.concatenate([wide[16 * g : 16 * g + 16] for g in range(4)], axis=1).astype(jnp.bfloat16)
        rbuf[core, yfull, pos["z"], pos["x"]] = tile

    def router_phase(phase, dims):
        at = {"x": pos["x"], "y": yfull, "z": pos["z"]}
        if phase == 3:
            return [(rbuf.at[core], partner)], rbuf.at[1 - core]
        known = dims[:phase]
        index = tuple(slice(None) if d in known else at[d] for d in "yzx")
        ref = rbuf.at[(core,) + index]
        dim = dims[phase]
        to = [y_device(lax.rem(yfull + k, 4)) for k in range(1, 4)] if dim == "y" else [
            device(dim, t) for t in peers_of(dim, pos)
        ]
        wide = tuple(pl.ds(0, 3) if d == dim else (slice(None) if d in known else 0) for d in "yzx")
        return [(ref, d) for d in to], rbuf.at[(core,) + wide]

    def router_step(done, start):
        for index, dims in enumerate(ROUTER_ORDER):

            @pl.when(core == index)
            def _():
                if done is not None:
                    _, view = router_phase(done, dims)
                    whole = pltpu.make_async_remote_copy(
                        view, view, rsend.at[done], rrecv.at[done], device_id=partner, device_id_type=MESH
                    )
                    whole.wait()
                if start is not None:
                    for ref, d in router_phase(start, dims)[0]:
                        pltpu.make_async_remote_copy(
                            ref, ref, rsend.at[start], rrecv.at[start], device_id=d, device_id_type=MESH
                        ).start()

    def copies(p, phase, ch):
        order = ORDER[p]
        dim = order[phase]
        part = pl.ds(starts[ch], chunks[ch])
        out = []
        for target in peers_of(dim, pos):
            if phase == 0:
                src, dst = S[p].at[part, target], R1[p].at[part, pos[dim]]
            elif phase == 1:
                src, dst = R1[p].at[part, :, target], R2[p].at[part, pos[dim]]
            else:
                src = R2[p].at[part, :, :, target]
                dst = R3[p].at[part, pos[dim]] if ch + 1 < count else LAST[p].at[:, pos[dim]]
            out.append(
                pltpu.make_async_remote_copy(
                    src, dst, send.at[0], recv.at[phase, ch], device_id=device(dim, target), device_id_type=MESH
                )
            )
        return out

    def merge(ch):
        loaded(ch)
        if ch + 2 < count:
            loads(ch + 2)

        def unit(j, _):
            for b in range(6):
                lanes = slice(LANES * b, LANES * (b + 1))
                turned = [
                    (mast[UNIT * j + i, :, lanes] + sec[UNIT * j + i, :, lanes].astype(jnp.float32)).T
                    for i in range(UNIT)
                ]
                for g in range(16):
                    group = 16 * b + g
                    to, p = group // 3, group % 3
                    at = {"x": to % 4, "y": (to // 4) % 2, "z": to // 8}
                    block = jnp.concatenate([t[8 * g : 8 * g + 8] for t in turned], axis=0).astype(jnp.bfloat16)
                    d0, d1, d2 = (at[d] for d in ORDER[p])
                    S[p][j, d0, d1, d2] = block
            return 0

        lax.fori_loop(starts[ch], starts[ch] + chunks[ch], unit, 0)

    def begin(phase, ch):
        for p in range(3):
            for cp in copies(p, phase, ch):
                cp.start()

        def unit(j, _):
            for p in range(3):
                own = pos[ORDER[p][phase]]
                if phase == 0:
                    R1[p][j, own] = S[p][j, own]
                elif phase == 1:
                    R2[p][j, own] = R1[p][j, :, own]
                elif ch + 1 < count:
                    R3[p][j, own] = R2[p][j, :, :, own]
                else:
                    LAST[p][j - starts[ch], own] = R2[p][j, :, :, own]
            return 0

        lax.fori_loop(starts[ch], starts[ch] + chunks[ch], unit, 0)

    def arrive(phase, ch):
        view = sec.at[pl.ds(starts[ch] * UNIT, chunks[ch] * UNIT), :, pl.ds(0, 512)]
        pltpu.make_async_copy(view, view, recv.at[phase, ch]).wait()

    def finish_router():
        def rows(i, _):
            z, y, x = i // 8, lax.rem(i // 4, 2), lax.rem(i, 4)
            tiles = [rbuf[k % 2, 2 * y + k // 2, z, x] for k in range(4)]
            for g in range(4):
                block = jnp.concatenate([w[:, 32 * g : 32 * g + 32] for w in tiles], axis=1)
                router[pl.ds(pl.multiple_of(64 * i + 16 * g, 16), 16), :] = block
            return 0

        lax.fori_loop(0, 32, rows, 0)

    merge(0)
    pl.semaphore_wait(barrier, len(greet))
    begin(0, 0)
    router_tile()
    router_step(None, 0)

    for t in range(1, count + 3):
        if t < count:
            merge(t)
            begin(0, t)
        if t <= count:
            arrive(0, t - 1)
            begin(1, t - 1)
        if 0 <= t - 2 < count:
            arrive(1, t - 2)
            begin(2, t - 2)
        if t in ROUTER_STEPS:
            phase = ROUTER_STEPS.index(t)
            router_step(phase, phase + 1 if phase < 3 else None)
            if phase == 3:
                finish_router()
        if t >= 3:
            arrive(2, t - 3)
            if t - 2 < count:
                assemble(starts[t - 3], chunks[t - 3], R3, gate, up)

    pltpu.make_async_copy(mast, mast, send.at[0]).wait()


def store_kernel(gate, up, router, e0, e1, e2, gate_out, up_out, router_out, gate_last, up_last, sem):
    done, last = gate.shape[0], gate_last.shape[0]
    copies = [
        pltpu.make_async_copy(gate, gate_out.at[pl.ds(0, done)], sem.at[0]),
        pltpu.make_async_copy(up, up_out.at[pl.ds(0, done)], sem.at[1]),
        pltpu.make_async_copy(router, router_out, sem.at[2]),
        pltpu.make_async_copy(gate_last, gate_out.at[pl.ds(done, last)], sem.at[3]),
        pltpu.make_async_copy(up_last, up_out.at[pl.ds(done, last)], sem.at[4]),
    ]
    for cp in copies[:3]:
        cp.start()
    assemble(0, last // UNIT, (e0, e1, e2), gate_last, up_last)
    for cp in copies[3:]:
        cp.start()
    for cp in copies:
        cp.wait()


def per_device(master_gate, second_gate, master_up, second_up, router_weight, router_gain):
    experts, rows, width = master_gate.shape
    units = experts // UNIT
    chunks = CHUNKS

    last = chunks[-1]

    def held(dims, count=units):
        return pltpu.VMEM((count,) + tuple(DIM[d] for d in dims) + (8 * UNIT, LANES), jnp.bfloat16)

    any_ = pl.BlockSpec(memory_space=pl.ANY)
    vmem = pl.BlockSpec(memory_space=pltpu.VMEM)
    shapes = [(experts, width // 32, rows * 32)] * 2 + [(rows * 32, 128)]
    outs = pl.pallas_call(
        lambda *refs: exchange_kernel(chunks, *refs),
        name="merge_exchange",
        out_shape=tuple(pltpu.VMEM((experts - UNIT * last,) + shape[1:], jnp.bfloat16) for shape in shapes[:2])
        + (pltpu.VMEM(shapes[2], jnp.bfloat16),)
        + tuple(held((o[2], o[1], o[0]), last) for o in ORDER),
        in_specs=[any_] * 6,
        out_specs=(vmem,) * 6,
        scratch_shapes=[held(o) for o in ORDER]
        + [held(o) for o in ORDER]
        + [held((o[1], o[0], o[2])) for o in ORDER]
        + [held((o[2], o[1], o[0]), units - last) for o in ORDER]
        + [
            pltpu.VMEM((experts, 2 * rows, width), jnp.float32),
            pltpu.VMEM((experts, 2 * rows, width), jnp.bfloat16),
            pltpu.VMEM((2, 4, 4, 4, 16, LANES), jnp.bfloat16),
            pltpu.VMEM((rows // 2, rows), jnp.float32),
            pltpu.VMEM((1, rows), jnp.float32),
            pltpu.SemaphoreType.DMA((1,)),
            pltpu.SemaphoreType.DMA((3, len(chunks))),
            pltpu.SemaphoreType.DMA((len(chunks), 2)),
            pltpu.SemaphoreType.DMA((2,)),
            pltpu.SemaphoreType.DMA((4,)),
            pltpu.SemaphoreType.DMA((4,)),
        ],
        compiler_params=pltpu.CompilerParams(
            collective_id=0, has_side_effects=True, vmem_limit_bytes=48 * 1024 * 1024
        ),
    )(master_gate, second_gate, master_up, second_up, router_weight.T, router_gain[None, :])
    return pl.pallas_call(
        store_kernel,
        name="store",
        out_shape=tuple(jax.ShapeDtypeStruct(shape, jnp.bfloat16) for shape in shapes),
        in_specs=[vmem] * 6,
        out_specs=(any_,) * 3,
        scratch_shapes=[pltpu.VMEM((UNIT * last,) + shape[1:], jnp.bfloat16) for shape in shapes[:2]]
        + [pltpu.SemaphoreType.DMA((5,))],
        compiler_params=pltpu.CompilerParams(vmem_limit_bytes=16 * 1024 * 1024),
    )(*(pltpu.with_memory_space_constraint(out, pltpu.VMEM) for out in outs))


def solution(mesh):
    placed = (
        P("expert", "shard", None),
        P("expert", "shard", None),
        P("expert", "shard", None),
        P("expert", "shard", None),
        P("shard", "expert"),
        P("shard"),
    )
    return jax.shard_map(
        per_device,
        mesh=mesh,
        in_specs=placed,
        out_specs=(P("expert", "shard", None), P("expert", "shard", None), P()),
        check_vma=False,
    )
```

```python
import jax
import jax.numpy as jnp
from jax import lax
from jax.experimental import pallas as pl
from jax.experimental.pallas import tpu as pltpu
from jax.sharding import PartitionSpec as P

MESH = pl.DeviceIdType.MESH
DIM = {"x": 4, "y": 2, "z": 4}
ORDER = (("x", "y", "z"), ("y", "z", "x"), ("z", "x", "y"))
UNIT = 2
CHUNKS = (2, 4, 4, 4, 2)
ROUTER_STEPS = (1, 3, 4, 5)
ROUTER_ORDER = (("x", "y", "z"), ("z", "y", "x"))
LANES = 128


def peers_of(dim, pos):
    return [lax.rem(pos[dim] + k, DIM[dim]) for k in ((2, 1, 3) if DIM[dim] == 4 else (1,))]


def assemble(first, units, pieces, gate, up):
    def unit(j, _):
        for p in range(3):
            for q in range(16):
                halves = []
                for src in (2 * q, 2 * q + 1):
                    at = {"x": src % 4, "y": (src // 4) % 2, "z": src // 8}
                    d0, d1, d2 = (at[d] for d in ORDER[p])
                    halves.append(pieces[p][j, d2, d1, d0])
                for out, cut in ((gate, slice(0, 64)), (up, slice(64, 128))):
                    whole = jnp.concatenate([h[:, cut] for h in halves], axis=1)
                    for i in range(UNIT):
                        out[UNIT * j + i, 8 * p : 8 * p + 8, LANES * q : LANES * (q + 1)] = whole[8 * i : 8 * i + 8]
        return 0

    lax.fori_loop(first, first + units, unit, 0)


def exchange_kernel(
    chunks, mg, sg, mu, su, rw, rg, gate, up, router, e0, e1, e2,
    s0, s1, s2, a0, a1, a2, b0, b1, b2, c0, c1, c2, mast, sec, rbuf, weight, gain, send, recv, load, rload, rsend, rrecv,
):
    count = len(chunks)
    starts = [sum(chunks[:c]) for c in range(count)]
    S, R1, R2, R3, LAST = (s0, s1, s2), (a0, a1, a2), (b0, b1, b2), (c0, c1, c2), (e0, e1, e2)
    e = lax.axis_index("expert")
    s = lax.axis_index("shard")
    core, y_lo = lax.rem(e, 2), e // 2
    pos = {"x": lax.rem(s, 4), "y": lax.rem(s // 4, 2), "z": s // 8}
    yfull = pos["y"] * 2 + y_lo

    def device(dim, target):
        q = dict(pos)
        q[dim] = target
        return (e, q["z"] * 8 + q["y"] * 4 + q["x"])

    def y_device(target):
        return (lax.rem(target, 2) * 2 + core, pos["z"] * 8 + (target // 2) * 4 + pos["x"])

    partner = (y_lo * 2 + 1 - core, s)

    def loads(ch):
        part = pl.ds(starts[ch] * UNIT, chunks[ch] * UNIT)
        for k, (m, t) in enumerate(((mg, sg), (mu, su))):
            rows = pl.ds(64 * k, 64)
            pltpu.make_async_copy(m.at[part], mast.at[part, rows], load.at[ch, 0]).start()
            pltpu.make_async_copy(t.at[part], sec.at[part, rows], load.at[ch, 1]).start()

    def loaded(ch):
        part = pl.ds(starts[ch] * UNIT, chunks[ch] * UNIT)
        pltpu.make_async_copy(mast.at[part], mast.at[part], load.at[ch, 0]).wait()
        pltpu.make_async_copy(sec.at[part], sec.at[part], load.at[ch, 1]).wait()

    small = [pltpu.make_async_copy(rw, weight, rload.at[0]), pltpu.make_async_copy(rg, gain, rload.at[1])]
    for cp in small:
        cp.start()
    loads(0)
    loads(1)

    barrier = pltpu.get_barrier_semaphore()
    greet = [device(d, t) for d in "xz" for t in peers_of(d, pos)]
    greet += [y_device(lax.rem(yfull + k, 4)) for k in range(1, 4)]
    greet.append(partner)
    for d in greet:
        pl.semaphore_signal(barrier, inc=1, device_id=d, device_id_type=MESH)

    def router_tile():
        for cp in small:
            cp.wait()
        wide = (weight[...] * gain[...]).T
        tile = jnp.concatenate([wide[16 * g : 16 * g + 16] for g in range(4)], axis=1).astype(jnp.bfloat16)
        rbuf[core, yfull, pos["z"], pos["x"]] = tile

    def router_phase(phase, dims):
        at = {"x": pos["x"], "y": yfull, "z": pos["z"]}
        if phase == 3:
            return [(rbuf.at[core], partner)], rbuf.at[1 - core]
        known = dims[:phase]
        index = tuple(slice(None) if d in known else at[d] for d in "yzx")
        ref = rbuf.at[(core,) + index]
        dim = dims[phase]
        to = [y_device(lax.rem(yfull + k, 4)) for k in range(1, 4)] if dim == "y" else [
            device(dim, t) for t in peers_of(dim, pos)
        ]
        wide = tuple(pl.ds(0, 3) if d == dim else (slice(None) if d in known else 0) for d in "yzx")
        return [(ref, d) for d in to], rbuf.at[(core,) + wide]

    def router_step(done, start):
        for index, dims in enumerate(ROUTER_ORDER):

            @pl.when(core == index)
            def _():
                if done is not None:
                    _, view = router_phase(done, dims)
                    whole = pltpu.make_async_remote_copy(
                        view, view, rsend.at[done], rrecv.at[done], device_id=partner, device_id_type=MESH
                    )
                    whole.wait()
                if start is not None:
                    for ref, d in router_phase(start, dims)[0]:
                        pltpu.make_async_remote_copy(
                            ref, ref, rsend.at[start], rrecv.at[start], device_id=d, device_id_type=MESH
                        ).start()

    def copies(p, phase, ch):
        order = ORDER[p]
        dim = order[phase]
        part = pl.ds(starts[ch], chunks[ch])
        out = []
        for target in peers_of(dim, pos):
            if phase == 0:
                src, dst = S[p].at[part, target], R1[p].at[part, pos[dim]]
            elif phase == 1:
                src, dst = R1[p].at[part, :, target], R2[p].at[part, pos[dim]]
            else:
                src = R2[p].at[part, :, :, target]
                dst = R3[p].at[part, pos[dim]] if ch + 1 < count else LAST[p].at[:, pos[dim]]
            out.append(
                pltpu.make_async_remote_copy(
                    src, dst, send.at[0], recv.at[phase, ch], device_id=device(dim, target), device_id_type=MESH
                )
            )
        return out

    def merge(ch):
        loaded(ch)
        if ch + 2 < count:
            loads(ch + 2)

        def unit(j, _):
            for b in range(6):
                lanes = slice(LANES * b, LANES * (b + 1))
                turned = [
                    (mast[UNIT * j + i, :, lanes] + sec[UNIT * j + i, :, lanes].astype(jnp.float32)).T
                    for i in range(UNIT)
                ]
                for g in range(16):
                    group = 16 * b + g
                    to, p = group // 3, group % 3
                    at = {"x": to % 4, "y": (to // 4) % 2, "z": to // 8}
                    block = jnp.concatenate([t[8 * g : 8 * g + 8] for t in turned], axis=0).astype(jnp.bfloat16)
                    d0, d1, d2 = (at[d] for d in ORDER[p])
                    S[p][j, d0, d1, d2] = block
            return 0

        lax.fori_loop(starts[ch], starts[ch] + chunks[ch], unit, 0)

    def begin(phase, ch):
        for p in range(3):
            for cp in copies(p, phase, ch):
                cp.start()

        def unit(j, _):
            for p in range(3):
                own = pos[ORDER[p][phase]]
                if phase == 0:
                    R1[p][j, own] = S[p][j, own]
                elif phase == 1:
                    R2[p][j, own] = R1[p][j, :, own]
                elif ch + 1 < count:
                    R3[p][j, own] = R2[p][j, :, :, own]
                else:
                    LAST[p][j - starts[ch], own] = R2[p][j, :, :, own]
            return 0

        lax.fori_loop(starts[ch], starts[ch] + chunks[ch], unit, 0)

    def arrive(phase, ch):
        view = sec.at[pl.ds(starts[ch] * UNIT, chunks[ch] * UNIT), :, pl.ds(0, 512)]
        pltpu.make_async_copy(view, view, recv.at[phase, ch]).wait()

    def finish_router():
        def rows(i, _):
            z, y, x = i // 8, lax.rem(i // 4, 2), lax.rem(i, 4)
            tiles = [rbuf[k % 2, 2 * y + k // 2, z, x] for k in range(4)]
            for g in range(4):
                block = jnp.concatenate([w[:, 32 * g : 32 * g + 32] for w in tiles], axis=1)
                router[pl.ds(pl.multiple_of(64 * i + 16 * g, 16), 16), :] = block
            return 0

        lax.fori_loop(0, 32, rows, 0)

    merge(0)
    pl.semaphore_wait(barrier, len(greet))
    begin(0, 0)
    router_tile()
    router_step(None, 0)

    for t in range(1, count + 3):
        if t < count:
            merge(t)
            begin(0, t)
        if t <= count:
            arrive(0, t - 1)
            begin(1, t - 1)
        if 0 <= t - 2 < count:
            arrive(1, t - 2)
            begin(2, t - 2)
        if t in ROUTER_STEPS:
            phase = ROUTER_STEPS.index(t)
            router_step(phase, phase + 1 if phase < 3 else None)
            if phase == 3:
                finish_router()
        if t >= 3:
            arrive(2, t - 3)
            if t - 2 < count:
                assemble(starts[t - 3], chunks[t - 3], R3, gate, up)

    pltpu.make_async_copy(mast, mast, send.at[0]).wait()


def store_kernel(gate, up, router, e0, e1, e2, gate_out, up_out, router_out, gate_last, up_last, sem):
    done, last = gate.shape[0], gate_last.shape[0]
    copies = [
        pltpu.make_async_copy(gate, gate_out.at[pl.ds(0, done)], sem.at[0]),
        pltpu.make_async_copy(up, up_out.at[pl.ds(0, done)], sem.at[1]),
        pltpu.make_async_copy(router, router_out, sem.at[2]),
        pltpu.make_async_copy(gate_last, gate_out.at[pl.ds(done, last)], sem.at[3]),
        pltpu.make_async_copy(up_last, up_out.at[pl.ds(done, last)], sem.at[4]),
    ]
    for cp in copies[:3]:
        cp.start()
    assemble(0, last // UNIT, (e0, e1, e2), gate_last, up_last)
    for cp in copies[3:]:
        cp.start()
    for cp in copies:
        cp.wait()


def per_device(master_gate, second_gate, master_up, second_up, router_weight, router_gain):
    experts, rows, width = master_gate.shape
    units = experts // UNIT
    chunks = CHUNKS

    last = chunks[-1]

    def held(dims, count=units):
        return pltpu.VMEM((count,) + tuple(DIM[d] for d in dims) + (8 * UNIT, LANES), jnp.bfloat16)

    any_ = pl.BlockSpec(memory_space=pl.ANY)
    vmem = pl.BlockSpec(memory_space=pltpu.VMEM)
    shapes = [(experts, width // 32, rows * 32)] * 2 + [(rows * 32, 128)]
    outs = pl.pallas_call(
        lambda *refs: exchange_kernel(chunks, *refs),
        name="merge_exchange",
        out_shape=tuple(pltpu.VMEM((experts - UNIT * last,) + shape[1:], jnp.bfloat16) for shape in shapes[:2])
        + (pltpu.VMEM(shapes[2], jnp.bfloat16),)
        + tuple(held((o[2], o[1], o[0]), last) for o in ORDER),
        in_specs=[any_] * 6,
        out_specs=(vmem,) * 6,
        scratch_shapes=[held(o) for o in ORDER]
        + [held(o) for o in ORDER]
        + [held((o[1], o[0], o[2])) for o in ORDER]
        + [held((o[2], o[1], o[0]), units - last) for o in ORDER]
        + [
            pltpu.VMEM((experts, 2 * rows, width), jnp.float32),
            pltpu.VMEM((experts, 2 * rows, width), jnp.bfloat16),
            pltpu.VMEM((2, 4, 4, 4, 16, LANES), jnp.bfloat16),
            pltpu.VMEM((rows // 2, rows), jnp.float32),
            pltpu.VMEM((1, rows), jnp.float32),
            pltpu.SemaphoreType.DMA((1,)),
            pltpu.SemaphoreType.DMA((3, len(chunks))),
            pltpu.SemaphoreType.DMA((len(chunks), 2)),
            pltpu.SemaphoreType.DMA((2,)),
            pltpu.SemaphoreType.DMA((4,)),
            pltpu.SemaphoreType.DMA((4,)),
        ],
        compiler_params=pltpu.CompilerParams(
            collective_id=0, has_side_effects=True, vmem_limit_bytes=48 * 1024 * 1024
        ),
    )(master_gate, second_gate, master_up, second_up, router_weight.T, router_gain[None, :])
    return pl.pallas_call(
        store_kernel,
        name="store",
        out_shape=tuple(jax.ShapeDtypeStruct(shape, jnp.bfloat16) for shape in shapes),
        in_specs=[vmem] * 6,
        out_specs=(any_,) * 3,
        scratch_shapes=[pltpu.VMEM((UNIT * last,) + shape[1:], jnp.bfloat16) for shape in shapes[:2]]
        + [pltpu.SemaphoreType.DMA((5,))],
        compiler_params=pltpu.CompilerParams(vmem_limit_bytes=16 * 1024 * 1024),
    )(*(pltpu.with_memory_space_constraint(out, pltpu.VMEM) for out in outs))


def solution(mesh):
    placed = (
        P("expert", "shard", None),
        P("expert", "shard", None),
        P("expert", "shard", None),
        P("expert", "shard", None),
        P("shard", "expert"),
        P("shard"),
    )
    return jax.shard_map(
        per_device,
        mesh=mesh,
        in_specs=placed,
        out_specs=(P("expert", "shard", None), P("expert", "shard", None), P()),
        check_vma=False,
    )
```
